512 devices in a mesh: angle: 2 (over y), row: 128 (over z, x), col: 2 (over core).
Axes of the slice: x: 4, y: 2, z: 32, core: 2. Of those that a mesh axis runs over, the one named last changes fastest.
The devices are a block of a 4x8x32 slice.
Arguments:
- obj_field: float32 [2, 32768, 1024], P(None, ('angle', 'row'), 'col'), parts along dimension 1, may hold values from -6 to 6
- probe_modes: bfloat16 [2, 6, 256, 256], replicated, may hold values from -6 to 6
- centers: int32 [512, 2], P(('angle', 'row', 'col')), parts along dimension 0, may hold values from 0 to 16383, as said below
- amplitudes: float32 [512, 256, 256], P(('angle', 'row', 'col')), parts along dimension 0, may hold values from 0.2 to 4
Outputs:
- new_object: float32 [2, 32768, 1024], P(None, ('angle', 'row'), 'col'), parts along dimension 1
- new_probe: float32 [2, 12, 256, 256], P(None, 'angle'), parts along dimension 1
The draws below stay inside these ranges and needn't reach their ends.
There are 2 independent parts, one for each index of `angle`. The reference program is written for one: setup_inputs(seed, part) draws one part's arguments, and reference() takes and returns one part's arrays. A program takes and returns all parts, laid end to end along the dimension named above; an argument that names none is the same for every part. Nothing has to cross between parts.
Inputs may be any that keep to these rules, and one draw needn't show every extreme that they name: `centers`: position k belongs to device d = k // 1 of the row+col order (row slowest); its centre lies in that device's tile: row in [(d // (1024 // 512)) * 128, + 128), column in [(d % (1024 // 512)) * 512, + 512).
All inputs are finite; a program needn't handle non-finite values.
Results may differ from the reference program's by a relative error of at most 0.0003.
Values sent between devices are 32-bit elements; how exact they have to be, the bound alone decides.
No kernel may reach another device: no remote copies, remote signals or barrier semaphores. Data moves between devices by JAX's collectives and lax.ppermute only.
A program may use at most 64 MiB of HBM per device.

```python
import math
import jax
import jax.numpy as jnp
from jax import lax

P_SIZE = 256
MODES = 6
TILE_R = 128
TILE_C = 512
POS_DEV = 1
OBJ_ROWS = 16384
OBJ_COLS = 1024
POSITIONS = 256


def draw_centers(key, part):
    first_key, second_key = jax.random.split(jax.random.fold_in(key, 11))
    owner = jnp.arange(POSITIONS, dtype=jnp.int32) // POS_DEV
    tiles_across = OBJ_COLS // TILE_C
    tile_row = owner // tiles_across
    tile_col = owner % tiles_across
    rows_drawn = tile_row * TILE_R + jax.random.randint(first_key, (POSITIONS,), 0, TILE_R)
    cols_drawn = tile_col * TILE_C + jax.random.randint(second_key, (POSITIONS,), 0, TILE_C)
    return jnp.stack([rows_drawn, cols_drawn], axis=1).astype(jnp.int32)


def steps_of(key, extent, cuts, smallest, largest):
    def one(axis_at, shards_of):
        steps = jax.random.uniform(jax.random.fold_in(jax.random.fold_in(key, 6), axis_at), (shards_of,), jnp.float32, smallest / len(cuts), largest / len(cuts))
        return jnp.repeat(jnp.exp(steps), extent[axis_at] // shards_of).reshape((-1,) + (1,) * (len(extent) - axis_at - 1))

    gain = one(*cuts[0])
    for cut in cuts[1:]:
        gain = gain * one(*cut)
    return gain


def scatter_about(own_key, extent, width, most, shards=(), kind=jnp.bfloat16):
    gain = steps_of(own_key, extent, shards, -0.22, 0.18) if shards else 1.0
    entries = jax.random.normal(own_key, extent, jnp.float32) * width * gain
    return jnp.minimum(jnp.maximum(entries, -most), most).astype(kind)


def setup_inputs(seed: int = 0, part: int = 0) -> dict:
    splits = jax.random.split(jax.random.key(seed), 5)
    own_keys = jax.random.split(jax.random.fold_in(splits[4], part), 5)
    return {
        "obj_field": scatter_about(own_keys[0], (2, OBJ_ROWS, OBJ_COLS), 1.0, 6.0, ((1, 128), (2, 2)), jnp.float32),
        "probe_modes": scatter_about(splits[1], (2, MODES, P_SIZE, P_SIZE), 1.0, 6.0),
        "centers": draw_centers(jax.random.fold_in(jax.random.fold_in(splits[4], part), 71), part),
        "amplitudes": jnp.clip(jnp.exp(math.log(4.0) - 2.9957323 * jax.random.uniform(own_keys[3], (POSITIONS, P_SIZE, P_SIZE), jnp.float32) ** steps_of(own_keys[3], (POSITIONS, P_SIZE, P_SIZE), ((0, 256),), -0.2, 0.2)), 0.2, 4.0),
    }


def reference(obj_field, probe_modes, centers, amplitudes):
    margin = P_SIZE // 2
    probe = probe_modes.astype(jnp.float32)
    probe_real = probe[0]
    probe_imag = probe[1]
    spot_map = lax.optimization_barrier(jnp.sum(probe_real * probe_real + probe_imag * probe_imag, axis=0))
    padded = jnp.pad(obj_field, ((0, 0), (margin, margin), (margin, margin)))
    anchor = jnp.zeros((), jnp.int32)

    def visit_position(totals, inputs):
        buffer, probe_grad, probe_weight = totals
        center, measured = inputs
        row_start = center[0].astype(jnp.int32)
        col_start = center[1].astype(jnp.int32)
        window = lax.dynamic_slice(padded, (anchor, row_start, col_start), (2, P_SIZE, P_SIZE))
        win_real = window[0]
        win_imag = window[1]
        exit_real = probe_real * win_real - probe_imag * win_imag
        exit_imag = probe_real * win_imag + probe_imag * win_real
        far_field = jnp.fft.fft2(lax.complex(exit_real, exit_imag), norm='ortho')
        far_real = jnp.real(far_field)
        far_imag = jnp.imag(far_field)
        modulus = jnp.sqrt(lax.optimization_barrier(jnp.sum(far_real * far_real + far_imag * far_imag, axis=0)))
        factor = measured / (modulus + 0.5)
        back_wave = jnp.fft.ifft2(lax.complex(far_real * factor, far_imag * factor), norm='ortho')
        diff_real = jnp.real(back_wave) - exit_real
        diff_imag = jnp.imag(back_wave) - exit_imag
        obj_real = lax.optimization_barrier(jnp.sum(probe_real * diff_real + probe_imag * diff_imag, axis=0))
        obj_imag = lax.optimization_barrier(jnp.sum(probe_real * diff_imag - probe_imag * diff_real, axis=0))
        stacked = jnp.stack([obj_real, obj_imag, spot_map])
        current = lax.dynamic_slice(buffer, (anchor, row_start, col_start), (3, P_SIZE, P_SIZE))
        buffer = lax.dynamic_update_slice(buffer, current + stacked, (anchor, row_start, col_start))
        probe_grad = probe_grad + jnp.stack([win_real * diff_real + win_imag * diff_imag, win_real * diff_imag - win_imag * diff_real])
        probe_weight = probe_weight + win_real * win_real + win_imag * win_imag
        return ((buffer, probe_grad, probe_weight), None)
    start_state = (jnp.zeros((3, OBJ_ROWS + 2 * margin, OBJ_COLS + 2 * margin), jnp.float32), jnp.zeros((2, MODES, P_SIZE, P_SIZE), jnp.float32), jnp.zeros((P_SIZE, P_SIZE), jnp.float32))
    final_state, unused = lax.scan(visit_position, start_state, (centers, amplitudes))
    buffer, probe_grad, probe_weight = final_state
    interior = buffer[:, margin:margin + OBJ_ROWS, margin:margin + OBJ_COLS]
    illumination = interior[2]
    peak_value = jnp.max(illumination)
    new_object = obj_field + interior[:2] / (illumination + 0.1 * peak_value)
    peak_weight = jnp.max(probe_weight)
    new_probe = probe + probe_grad / (probe_weight + 0.1 * peak_weight)
    return (new_object, new_probe)
```

```python
import functools
import math

import jax
import jax.numpy as jnp
import numpy as np
from jax import lax
from jax.experimental import pallas as pl
from jax.experimental.pallas import tpu as pltpu
from jax.sharding import Mesh
from jax.sharding import PartitionSpec as P


ROW = ("row_0", "row_1", "row_2")
ROW_COL = ROW + ("col",)
ANGLE_ROW = ("angle",) + ROW
ANGLE_ROW_COL = ANGLE_ROW + ("col",)
TILE = (8, 128)


def partners(row_step, swap):
    rows = math.prod(lax.axis_size(axis) for axis in ROW)
    cols = lax.axis_size("col")
    assert cols == 2
    return [
        (row * cols + col, (row + row_step) * cols + (1 - col if swap else col))
        for row in range(rows)
        for col in range(cols)
        if 0 <= row + row_step < rows
    ]


def extended_tile(block, margin):
    rows, cols = block.shape[1:]
    assert rows == margin
    left_col = lax.axis_index("col") == 0
    edge = jnp.where(left_col, block[:, :, cols - margin :], block[:, :, :margin])
    above = lax.ppermute(block, ROW_COL, partners(1, False))
    below = lax.ppermute(block, ROW_COL, partners(-1, False))
    edge_above = lax.ppermute(edge, ROW_COL, partners(1, True))
    edge_below = lax.ppermute(edge, ROW_COL, partners(-1, True))
    beside = lax.ppermute(edge, ROW_COL, partners(0, True))
    middle = jnp.concatenate([above, block, below], axis=1)
    side = jnp.concatenate([edge_above, beside, edge_below], axis=1)
    zero = jnp.zeros_like(side)
    return jnp.concatenate(
        [jnp.where(left_col, zero, side), middle, jnp.where(left_col, side, zero)], axis=2
    )


def folded_tile(buffer, margin):
    cols = buffer.shape[2] - 2 * margin
    left_col = lax.axis_index("col") == 0
    middle = buffer[:, :, margin : margin + cols]
    side = jnp.where(left_col, buffer[:, :, margin + cols :], buffer[:, :, :margin])
    up, own, down = (slice(k * margin, (k + 1) * margin) for k in range(3))
    from_below = lax.ppermute(middle[:, up], ROW_COL, partners(-1, False))
    from_above = lax.ppermute(middle[:, down], ROW_COL, partners(1, False))
    edge = (
        lax.ppermute(side[:, up], ROW_COL, partners(-1, True))
        + lax.ppermute(side[:, down], ROW_COL, partners(1, True))
        + lax.ppermute(side[:, own], ROW_COL, partners(0, True))
    )
    rest = jnp.zeros(edge.shape[:2] + (cols - margin,), edge.dtype)
    edges = jnp.where(
        left_col,
        jnp.concatenate([rest, edge], axis=2),
        jnp.concatenate([edge, rest], axis=2),
    )
    return middle[:, own] + from_below + from_above + edges


def dft_tables(side):
    index = np.arange(side)
    phase = (index[:, None] * index[None, :] % side) * (2.0 * math.pi / side)
    cosine, sine = np.cos(phase) / math.sqrt(side), np.sin(phase) / math.sqrt(side)
    both = np.block([[cosine, sine], [-sine, cosine]])
    out = []
    for table in (both, both.T):
        head = table.astype(jnp.bfloat16)
        out.append((head, (table - head.astype(np.float64)).astype(jnp.bfloat16)))
    return out


def split(x):
    head = x.astype(jnp.bfloat16)
    return head, (x - head.astype(jnp.float32)).astype(jnp.bfloat16)


def right_dot(x, table):
    head, rest = split(x)
    return jnp.dot(
        jnp.concatenate([head, rest, head], axis=1),
        jnp.concatenate([table[0], table[0], table[1]], axis=0),
        preferred_element_type=jnp.float32,
    )


def left_dot(table, x):
    head, rest = split(x)
    return jnp.dot(
        jnp.concatenate([table[0], table[0], table[1]], axis=1),
        jnp.concatenate([head, rest, head], axis=0),
        preferred_element_type=jnp.float32,
    )


def wave_kernel(column, win, probe, amp, forward, inverse, obj, kept, sent, far, factor):
    modes, side = probe.shape[1], probe.shape[2]
    left_col = column[0] == 0
    tiles = side // 8

    def exit_wave(m):
        probe_real = probe[0, m].astype(jnp.float32)
        probe_imag = probe[1, m].astype(jnp.float32)
        exit_real = probe_real * win[0] - probe_imag * win[1]
        exit_imag = probe_real * win[1] + probe_imag * win[0]
        return probe_real, probe_imag, exit_real, exit_imag

    def transform(real, imag, right, left):
        mixed = right_dot(jnp.concatenate([real, imag], axis=1), right)
        return left_dot(left, jnp.concatenate([mixed[:, :side], mixed[:, side:]], axis=0))

    def put(base, first, second):
        where = pl.ds(base, tiles)
        kept[where] = jnp.where(left_col, first, second).reshape((tiles,) + TILE)
        sent[where] = jnp.where(left_col, second, first).reshape((tiles,) + TILE)

    factor[...] = jnp.zeros_like(factor)

    @pl.loop(0, modes)
    def _(m):
        _, _, exit_real, exit_imag = exit_wave(m)
        out = transform(exit_real, exit_imag, inverse, forward)
        far[m] = out
        factor[...] += out[:side] * out[:side] + out[side:] * out[side:]

    factor[...] = amp[...] / (jnp.sqrt(factor[...]) + 0.5)
    obj[...] = jnp.zeros_like(obj)

    @pl.loop(0, modes)
    def _(m):
        scale = factor[...]
        back = transform(far[m, :side] * scale, far[m, side:] * scale, forward, inverse)
        probe_real, probe_imag, exit_real, exit_imag = exit_wave(m)
        diff_real = back[:side] - exit_real
        diff_imag = back[side:] - exit_imag
        obj[0] += probe_real * diff_real + probe_imag * diff_imag
        obj[1] += probe_real * diff_imag - probe_imag * diff_real
        obj[2] += probe_real * probe_real + probe_imag * probe_imag
        grad_real = win[0] * diff_real + win[1] * diff_imag
        grad_imag = win[0] * diff_imag - win[1] * diff_real
        for half in range(side // 128):
            cols = slice(128 * half, 128 * half + 128)
            put((m * (side // 128) + half) * tiles, grad_real[:, cols], grad_imag[:, cols])

    weight = win[0] * win[0] + win[1] * win[1]
    put(modes * (side // 128) * tiles, weight[:, :128], weight[:, 128:])


def waves(column, window, probe, amplitude):
    modes, side = probe.shape[1], probe.shape[2]
    assert side == 256
    forward, inverse = (jnp.asarray(np.stack(table)) for table in dft_tables(side))
    flops = 4 * modes * 2 * side * (6 * side) * (2 * side)
    half = jax.ShapeDtypeStruct(((2 * modes + 1) * (side // 8),) + TILE, jnp.float32)
    vmem = pl.BlockSpec(memory_space=pltpu.VMEM)
    return pl.pallas_call(
        wave_kernel,
        name="waves",
        out_shape=(jax.ShapeDtypeStruct((3, side, side), jnp.float32), half, half),
        in_specs=[pl.BlockSpec(memory_space=pltpu.SMEM)] + [vmem] * 5,
        out_specs=(vmem, vmem, vmem),
        scratch_shapes=[
            pltpu.VMEM((modes, 2 * side, side), jnp.float32),
            pltpu.VMEM((side, side), jnp.float32),
        ],
        compiler_params=pltpu.CompilerParams(vmem_limit_bytes=40 * 1024 * 1024),
        cost_estimate=pl.CostEstimate(
            flops=flops, bytes_accessed=12 * 1024 * 1024, transcendentals=0
        ),
    )(column, window, probe, amplitude, forward, inverse)


def probe_kernel(column, own, other, probe, out):
    modes, side = probe.shape[1], probe.shape[2]
    left_col = column[0] == 0
    chunk = own.shape[1] - 1
    group = math.gcd(chunk, side // 8)

    def halves(tile):
        where = (tile // chunk, slice(tile % chunk, tile % chunk + group))
        mine, theirs = (ref[where].reshape(8 * group, 128) for ref in (own, other))
        return jnp.where(left_col, mine, theirs), jnp.where(left_col, theirs, mine)

    per_half = side // 8
    groups = per_half // group
    base = 2 * modes * per_half
    weight = [halves(base + j * group) for j in range(groups)]
    peak = functools.reduce(jnp.maximum, [jnp.max(w) for pair in weight for w in pair])
    for j in range(groups):
        rows = slice(8 * group * j, 8 * group * (j + 1))
        for half in range(2):
            inverse = 1.0 / (weight[j][half] + 0.1 * peak)
            cols = slice(128 * half, 128 * half + 128)
            for m in range(modes):
                grads = halves((2 * m + half) * per_half + j * group)
                for part in range(2):
                    out[part, m, rows, cols] = (
                        probe[part, m, rows, cols].astype(jnp.float32) + grads[part] * inverse
                    )


def probe_update(column, own, other, probe):
    vmem = pl.BlockSpec(memory_space=pltpu.VMEM)
    return pl.pallas_call(
        probe_kernel,
        name="probe_update",
        out_shape=jax.ShapeDtypeStruct(probe.shape, jnp.float32),
        in_specs=[pl.BlockSpec(memory_space=pltpu.SMEM)] + [vmem] * 3,
        out_specs=vmem,
        compiler_params=pltpu.CompilerParams(vmem_limit_bytes=40 * 1024 * 1024),
        cost_estimate=pl.CostEstimate(
            flops=4 * probe.size, bytes_accessed=9 * probe.size, transcendentals=0
        ),
    )(column, own, other, probe)


def exchange(chunks, axis):
    return lax.all_to_all(chunks, axis, 0, 0, tiled=True)


def scatter_sum(tiles, axis):
    count = lax.axis_size(axis)
    part = -(-tiles.shape[0] // count)
    tiles = jnp.pad(tiles, ((0, part * count - tiles.shape[0]), (0, 0), (0, 0)))
    return jnp.sum(exchange(tiles.reshape((count, part) + TILE), axis), axis=0)


def gather(tiles, peak, axis):
    count = lax.axis_size(axis)
    tagged = jnp.concatenate([tiles, peak])
    return exchange(jnp.broadcast_to(tagged, (count,) + tagged.shape), axis)


def sum_and_peak(kept, sent, local_peak):
    swap = [(0, 1), (1, 0)]
    tiles = kept + lax.ppermute(sent, "col", swap)
    counts = []
    for axis in ROW[::-1]:
        counts.append(tiles.shape[0])
        tiles = scatter_sum(tiles, axis)
    peak = jnp.full((1,) + TILE, local_peak)
    for axis, count in zip(ROW, counts[::-1], strict=True):
        got = gather(tiles, peak, axis)
        peak = jnp.max(got[:, -1:], axis=0)
        tiles = got[:, :-1].reshape((-1,) + TILE)[:count]
    other = lax.ppermute(got, "col", swap)
    peak = jnp.maximum(peak, jnp.max(other[:, -1:], axis=0))
    return got, other, peak[0, 0, 0]


def local(obj_field, probe_modes, centers, amplitudes):
    tile_rows, tile_cols = obj_field.shape[1:]
    side = probe_modes.shape[2]
    margin = side // 2
    start_row = centers[0, 0] - lax.axis_index(ROW) * tile_rows
    start_col = centers[0, 1] - lax.axis_index("col") * tile_cols
    zero = jnp.zeros((), jnp.int32)
    column = lax.axis_index("col").astype(jnp.int32).reshape(1)
    extended = extended_tile(obj_field, margin)
    window = lax.dynamic_slice(extended, (zero, start_row, start_col), (2, side, side))
    stacked, kept, sent = waves(column, window, probe_modes, amplitudes[0])
    buffer = lax.dynamic_update_slice(
        jnp.zeros((3, tile_rows + 2 * margin, tile_cols + 2 * margin), jnp.float32),
        stacked,
        (zero, start_row, start_col),
    )
    folded = folded_tile(buffer, margin)
    illumination = folded[2]
    own, other, peak = sum_and_peak(kept, sent, jnp.max(illumination))
    new_object = obj_field + folded[:2] / (illumination + 0.1 * peak)
    return new_object, probe_update(column, own, other, probe_modes)


def solution(mesh):
    near, middle = 4, min(4, mesh.shape["row"] // 4)
    rows = mesh.shape["row"]
    split_mesh = Mesh(
        mesh.devices.reshape(
            mesh.shape["angle"], rows // (near * middle), middle, near, mesh.shape["col"]
        ),
        ANGLE_ROW_COL,
    )
    return jax.shard_map(
        local,
        mesh=split_mesh,
        in_specs=(
            P(None, ANGLE_ROW, "col"),
            P(),
            P(ANGLE_ROW_COL, None),
            P(ANGLE_ROW_COL, None, None),
        ),
        out_specs=(P(None, ANGLE_ROW, "col"), P(None, "angle", None, None)),
        check_vma=False,
    )
```

```python
import functools
import math

import jax
import jax.numpy as jnp
import numpy as np
from jax import lax
from jax.experimental import pallas as pl
from jax.experimental.pallas import tpu as pltpu
from jax.sharding import Mesh
from jax.sharding import PartitionSpec as P


ROW = ("row_0", "row_1", "row_2")
ROW_COL = ROW + ("col",)
ANGLE_ROW = ("angle",) + ROW
ANGLE_ROW_COL = ANGLE_ROW + ("col",)
TILE = (8, 128)


def partners(row_step, swap):
    rows = math.prod(lax.axis_size(axis) for axis in ROW)
    cols = lax.axis_size("col")
    assert cols == 2
    return [
        (row * cols + col, (row + row_step) * cols + (1 - col if swap else col))
        for row in range(rows)
        for col in range(cols)
        if 0 <= row + row_step < rows
    ]


def extended_tile(block, margin):
    rows, cols = block.shape[1:]
    assert rows == margin
    left_col = lax.axis_index("col") == 0
    edge = jnp.where(left_col, block[:, :, cols - margin :], block[:, :, :margin])
    above = lax.ppermute(block, ROW_COL, partners(1, False))
    below = lax.ppermute(block, ROW_COL, partners(-1, False))
    edge_above = lax.ppermute(edge, ROW_COL, partners(1, True))
    edge_below = lax.ppermute(edge, ROW_COL, partners(-1, True))
    beside = lax.ppermute(edge, ROW_COL, partners(0, True))
    middle = jnp.concatenate([above, block, below], axis=1)
    side = jnp.concatenate([edge_above, beside, edge_below], axis=1)
    zero = jnp.zeros_like(side)
    return jnp.concatenate(
        [jnp.where(left_col, zero, side), middle, jnp.where(left_col, side, zero)], axis=2
    )


def place_kernel(start, column, stacked, up, own, down, side, buffer):
    channels, height, width = stacked.shape
    rows, cols = own.shape[1:]
    left_col = column[0] == 0
    shift = lax.rem(start[1], 128)
    where = pl.ds(pl.multiple_of(start[1] - shift, 128), width + 128)
    buffer[...] = jnp.zeros_like(buffer)

    @pl.loop(0, channels)
    def _(k):
        tall = jnp.concatenate([stacked[k], jnp.zeros((rows, width), jnp.float32)], axis=0)
        tall = pltpu.roll(tall, start[0], 0)
        wide = jnp.concatenate([tall, jnp.zeros((height + rows, 128), jnp.float32)], axis=1)
        buffer[:, where] = pltpu.roll(wide, shift, 1)
        up[k] = buffer[:rows, rows : rows + cols]
        own[k] = buffer[rows : 2 * rows, rows : rows + cols]
        down[k] = buffer[2 * rows :, rows : rows + cols]
        side[k] = jnp.where(left_col, buffer[:, rows + cols :], buffer[:, :rows])


def place(start, column, stacked, rows, cols):
    channels, height, width = stacked.shape
    assert height == width == 2 * rows and rows == 128
    smem = pl.BlockSpec(memory_space=pltpu.SMEM)
    vmem = pl.BlockSpec(memory_space=pltpu.VMEM)
    part = jax.ShapeDtypeStruct((channels, rows, cols), jnp.float32)
    return pl.pallas_call(
        place_kernel,
        name="place",
        out_shape=(part, part, part, jax.ShapeDtypeStruct((channels, 3 * rows, rows), jnp.float32)),
        in_specs=[smem, smem, vmem],
        out_specs=(vmem,) * 4,
        scratch_shapes=[pltpu.VMEM((3 * rows, cols + 2 * rows), jnp.float32)],
        compiler_params=pltpu.CompilerParams(vmem_limit_bytes=24 * 1024 * 1024),
        cost_estimate=pl.CostEstimate(
            flops=20 * part.size, bytes_accessed=24 * part.size, transcendentals=0
        ),
    )(start, column, stacked)


def folded_tile(pieces):
    up, own, down, side = pieces
    rows, cols = own.shape[1:]
    left_col = lax.axis_index("col") == 0
    got = lax.ppermute(side, ROW_COL, partners(0, True))
    rest = jnp.zeros(got.shape[:2] + (cols - rows,), got.dtype)
    got = jnp.where(
        left_col, jnp.concatenate([rest, got], axis=2), jnp.concatenate([got, rest], axis=2)
    )
    up, own, down = (
        piece + got[:, k * rows : (k + 1) * rows] for k, piece in enumerate((up, own, down))
    )
    from_below = lax.ppermute(up, ROW_COL, partners(-1, False))
    from_above = lax.ppermute(down, ROW_COL, partners(1, False))
    return own + from_below + from_above


def dft_tables(side):
    index = np.arange(side)
    phase = (index[:, None] * index[None, :] % side) * (2.0 * math.pi / side)
    cosine, sine = np.cos(phase) / math.sqrt(side), np.sin(phase) / math.sqrt(side)
    both = np.block([[cosine, sine], [-sine, cosine]])
    out = []
    for table in (both, both.T):
        head = table.astype(jnp.bfloat16)
        out.append((head, (table - head.astype(np.float64)).astype(jnp.bfloat16)))
    return out


def split(x):
    head = x.astype(jnp.bfloat16)
    return head, (x - head.astype(jnp.float32)).astype(jnp.bfloat16)


def right_dot(x, table):
    head, rest = split(x)
    return jnp.dot(
        jnp.concatenate([head, rest, head], axis=1),
        jnp.concatenate([table[0], table[0], table[1]], axis=0),
        preferred_element_type=jnp.float32,
    )


def left_dot(table, x):
    head, rest = split(x)
    return jnp.dot(
        jnp.concatenate([table[0], table[0], table[1]], axis=1),
        jnp.concatenate([head, rest, head], axis=0),
        preferred_element_type=jnp.float32,
    )


def wave_kernel(column, win, probe, amp, forward, inverse, obj, kept, sent, far, factor):
    modes, side = probe.shape[1], probe.shape[2]
    left_col = column[0] == 0
    tiles = side // 8

    def exit_wave(m):
        probe_real = probe[0, m].astype(jnp.float32)
        probe_imag = probe[1, m].astype(jnp.float32)
        exit_real = probe_real * win[0] - probe_imag * win[1]
        exit_imag = probe_real * win[1] + probe_imag * win[0]
        return probe_real, probe_imag, exit_real, exit_imag

    def transform(real, imag, right, left):
        mixed = right_dot(jnp.concatenate([real, imag], axis=1), right)
        return left_dot(left, jnp.concatenate([mixed[:, :side], mixed[:, side:]], axis=0))

    def put(base, first, second):
        where = pl.ds(base, tiles)
        kept[where] = jnp.where(left_col, first, second).reshape((tiles,) + TILE)
        sent[where] = jnp.where(left_col, second, first).reshape((tiles,) + TILE)

    factor[...] = jnp.zeros_like(factor)

    @pl.loop(0, modes)
    def _(m):
        _, _, exit_real, exit_imag = exit_wave(m)
        out = transform(exit_real, exit_imag, inverse, forward)
        far[m] = out
        factor[...] += out[:side] * out[:side] + out[side:] * out[side:]

    factor[...] = amp[...] / (jnp.sqrt(factor[...]) + 0.5)
    obj[...] = jnp.zeros_like(obj)

    @pl.loop(0, modes)
    def _(m):
        scale = factor[...]
        back = transform(far[m, :side] * scale, far[m, side:] * scale, forward, inverse)
        probe_real, probe_imag, exit_real, exit_imag = exit_wave(m)
        diff_real = back[:side] - exit_real
        diff_imag = back[side:] - exit_imag
        obj[0] += probe_real * diff_real + probe_imag * diff_imag
        obj[1] += probe_real * diff_imag - probe_imag * diff_real
        obj[2] += probe_real * probe_real + probe_imag * probe_imag
        grad_real = win[0] * diff_real + win[1] * diff_imag
        grad_imag = win[0] * diff_imag - win[1] * diff_real
        for half in range(side // 128):
            cols = slice(128 * half, 128 * half + 128)
            put((m * (side // 128) + half) * tiles, grad_real[:, cols], grad_imag[:, cols])

    weight = win[0] * win[0] + win[1] * win[1]
    put(modes * (side // 128) * tiles, weight[:, :128], weight[:, 128:])


def waves(column, window, probe, amplitude):
    modes, side = probe.shape[1], probe.shape[2]
    assert side == 256
    forward, inverse = (jnp.asarray(np.stack(table)) for table in dft_tables(side))
    flops = 4 * modes * 2 * side * (6 * side) * (2 * side)
    half = jax.ShapeDtypeStruct(((2 * modes + 1) * (side // 8),) + TILE, jnp.float32)
    vmem = pl.BlockSpec(memory_space=pltpu.VMEM)
    return pl.pallas_call(
        wave_kernel,
        name="waves",
        out_shape=(jax.ShapeDtypeStruct((3, side, side), jnp.float32), half, half),
        in_specs=[pl.BlockSpec(memory_space=pltpu.SMEM)] + [vmem] * 5,
        out_specs=(vmem, vmem, vmem),
        scratch_shapes=[
            pltpu.VMEM((modes, 2 * side, side), jnp.float32),
            pltpu.VMEM((side, side), jnp.float32),
        ],
        compiler_params=pltpu.CompilerParams(vmem_limit_bytes=40 * 1024 * 1024),
        cost_estimate=pl.CostEstimate(
            flops=flops, bytes_accessed=12 * 1024 * 1024, transcendentals=0
        ),
    )(column, window, probe, amplitude, forward, inverse)


def probe_kernel(column, own, other, probe, out):
    modes, side = probe.shape[1], probe.shape[2]
    left_col = column[0] == 0
    chunk = own.shape[1] - 1
    group = math.gcd(chunk, side // 8)

    def halves(tile):
        where = (tile // chunk, slice(tile % chunk, tile % chunk + group))
        mine, theirs = (ref[where].reshape(8 * group, 128) for ref in (own, other))
        return jnp.where(left_col, mine, theirs), jnp.where(left_col, theirs, mine)

    per_half = side // 8
    groups = per_half // group
    base = 2 * modes * per_half
    weight = [halves(base + j * group) for j in range(groups)]
    peak = functools.reduce(jnp.maximum, [jnp.max(w) for pair in weight for w in pair])
    for j in range(groups):
        rows = slice(8 * group * j, 8 * group * (j + 1))
        for half in range(2):
            inverse = 1.0 / (weight[j][half] + 0.1 * peak)
            cols = slice(128 * half, 128 * half + 128)
            for m in range(modes):
                grads = halves((2 * m + half) * per_half + j * group)
                for part in range(2):
                    out[part, m, rows, cols] = (
                        probe[part, m, rows, cols].astype(jnp.float32) + grads[part] * inverse
                    )


def probe_update(column, own, other, probe):
    vmem = pl.BlockSpec(memory_space=pltpu.VMEM)
    return pl.pallas_call(
        probe_kernel,
        name="probe_update",
        out_shape=jax.ShapeDtypeStruct(probe.shape, jnp.float32),
        in_specs=[pl.BlockSpec(memory_space=pltpu.SMEM)] + [vmem] * 3,
        out_specs=vmem,
        compiler_params=pltpu.CompilerParams(vmem_limit_bytes=40 * 1024 * 1024),
        cost_estimate=pl.CostEstimate(
            flops=4 * probe.size, bytes_accessed=9 * probe.size, transcendentals=0
        ),
    )(column, own, other, probe)


def exchange(chunks, axis):
    return lax.all_to_all(chunks, axis, 0, 0, tiled=True)


def scatter_sum(tiles, axis):
    count = lax.axis_size(axis)
    part = -(-tiles.shape[0] // count)
    tiles = jnp.pad(tiles, ((0, part * count - tiles.shape[0]), (0, 0), (0, 0)))
    return jnp.sum(exchange(tiles.reshape((count, part) + TILE), axis), axis=0)


def gather(tiles, peak, axis):
    count = lax.axis_size(axis)
    tagged = jnp.concatenate([tiles, peak])
    return exchange(jnp.broadcast_to(tagged, (count,) + tagged.shape), axis)


def sum_and_peak(kept, sent, local_peak):
    swap = [(0, 1), (1, 0)]
    tiles = kept + lax.ppermute(sent, "col", swap)
    counts = []
    for axis in ROW[::-1]:
        counts.append(tiles.shape[0])
        tiles = scatter_sum(tiles, axis)
    peak = jnp.full((1,) + TILE, local_peak)
    for axis, count in zip(ROW, counts[::-1], strict=True):
        got = gather(tiles, peak, axis)
        peak = jnp.max(got[:, -1:], axis=0)
        tiles = got[:, :-1].reshape((-1,) + TILE)[:count]
    other = lax.ppermute(got, "col", swap)
    peak = jnp.maximum(peak, jnp.max(other[:, -1:], axis=0))
    return got, other, peak[0, 0, 0]


def update(obj_field, probe_modes, centers, amplitudes):
    tile_rows, tile_cols = obj_field.shape[1:]
    side = probe_modes.shape[2]
    margin = side // 2
    start_row = centers[0, 0] - lax.axis_index(ROW) * tile_rows
    start_col = centers[0, 1] - lax.axis_index("col") * tile_cols
    zero = jnp.zeros((), jnp.int32)
    column = lax.axis_index("col").astype(jnp.int32).reshape(1)
    extended = extended_tile(obj_field, margin)
    window = lax.dynamic_slice(extended, (zero, start_row, start_col), (2, side, side))
    stacked, kept, sent = waves(column, window, probe_modes, amplitudes[0])
    start = jnp.stack([start_row, start_col])
    folded = folded_tile(place(start, column, stacked, tile_rows, tile_cols))
    illumination = folded[2]
    own, other, peak = sum_and_peak(kept, sent, jnp.max(illumination))
    new_object = obj_field + folded[:2] / (illumination + 0.1 * peak)
    return new_object, probe_update(column, own, other, probe_modes)


def solution(mesh):
    near, middle = 4, min(4, mesh.shape["row"] // 4)
    rows = mesh.shape["row"]
    split_mesh = Mesh(
        mesh.devices.reshape(
            mesh.shape["angle"], rows // (near * middle), middle, near, mesh.shape["col"]
        ),
        ANGLE_ROW_COL,
    )
    return jax.shard_map(
        update,
        mesh=split_mesh,
        in_specs=(
            P(None, ANGLE_ROW, "col"),
            P(),
            P(ANGLE_ROW_COL, None),
            P(ANGLE_ROW_COL, None, None),
        ),
        out_specs=(P(None, ANGLE_ROW, "col"), P(None, "angle", None, None)),
        check_vma=False,
    )
```

```python
import functools
import math

import jax
import jax.numpy as jnp
import numpy as np
from jax import lax
from jax.experimental import pallas as pl
from jax.experimental.pallas import tpu as pltpu
from jax.sharding import Mesh
from jax.sharding import PartitionSpec as P


ROW = ("row_0", "row_1")
ROW_COL = ROW + ("col",)
ANGLE_ROW = ("angle",) + ROW
ANGLE_ROW_COL = ANGLE_ROW + ("col",)
NEAR = 8
TILE = (8, 128)


def partners(row_step, swap):
    rows = math.prod(lax.axis_size(axis) for axis in ROW)
    cols = lax.axis_size("col")
    assert cols == 2
    return [
        (row * cols + col, (row + row_step) * cols + (1 - col if swap else col))
        for row in range(rows)
        for col in range(cols)
        if 0 <= row + row_step < rows
    ]


def extended_tile(block, margin):
    rows, cols = block.shape[1:]
    assert rows == margin
    left_col = lax.axis_index("col") == 0
    edge = jnp.where(left_col, block[:, :, cols - margin :], block[:, :, :margin])
    above = lax.ppermute(block, ROW_COL, partners(1, False))
    below = lax.ppermute(block, ROW_COL, partners(-1, False))
    edge_above = lax.ppermute(edge, ROW_COL, partners(1, True))
    edge_below = lax.ppermute(edge, ROW_COL, partners(-1, True))
    beside = lax.ppermute(edge, ROW_COL, partners(0, True))
    middle = jnp.concatenate([above, block, below], axis=1)
    side = jnp.concatenate([edge_above, beside, edge_below], axis=1)
    zero = jnp.zeros_like(side)
    return jnp.concatenate(
        [jnp.where(left_col, zero, side), middle, jnp.where(left_col, side, zero)], axis=2
    )


def place_kernel(start, column, stacked, up, own, down, side, buffer):
    channels, height, width = stacked.shape
    rows, cols = own.shape[1:]
    left_col = column[0] == 0
    shift = lax.rem(start[1], 128)
    where = pl.ds(pl.multiple_of(start[1] - shift, 128), width + 128)
    buffer[...] = jnp.zeros_like(buffer)

    @pl.loop(0, channels)
    def _(k):
        tall = jnp.concatenate([stacked[k], jnp.zeros((rows, width), jnp.float32)], axis=0)
        tall = pltpu.roll(tall, start[0], 0)
        wide = jnp.concatenate([tall, jnp.zeros((height + rows, 128), jnp.float32)], axis=1)
        buffer[:, where] = pltpu.roll(wide, shift, 1)
        up[k] = buffer[:rows, rows : rows + cols]
        own[k] = buffer[rows : 2 * rows, rows : rows + cols]
        down[k] = buffer[2 * rows :, rows : rows + cols]
        side[k] = jnp.where(left_col, buffer[:, rows + cols :], buffer[:, :rows])


def place(start, column, stacked, rows, cols):
    channels, height, width = stacked.shape
    assert height == width == 2 * rows and rows == 128
    smem = pl.BlockSpec(memory_space=pltpu.SMEM)
    vmem = pl.BlockSpec(memory_space=pltpu.VMEM)
    part = jax.ShapeDtypeStruct((channels, rows, cols), jnp.float32)
    return pl.pallas_call(
        place_kernel,
        name="place",
        out_shape=(part, part, part, jax.ShapeDtypeStruct((channels, 3 * rows, rows), jnp.float32)),
        in_specs=[smem, smem, vmem],
        out_specs=(vmem,) * 4,
        scratch_shapes=[pltpu.VMEM((3 * rows, cols + 2 * rows), jnp.float32)],
        compiler_params=pltpu.CompilerParams(vmem_limit_bytes=24 * 1024 * 1024),
        cost_estimate=pl.CostEstimate(
            flops=20 * part.size, bytes_accessed=24 * part.size, transcendentals=0
        ),
    )(start, column, stacked)


def folded_tile(pieces):
    up, own, down, side = pieces
    rows, cols = own.shape[1:]
    left_col = lax.axis_index("col") == 0
    got = lax.ppermute(side, ROW_COL, partners(0, True))
    rest = jnp.zeros(got.shape[:2] + (cols - rows,), got.dtype)
    got = jnp.where(
        left_col, jnp.concatenate([rest, got], axis=2), jnp.concatenate([got, rest], axis=2)
    )
    up, own, down = (
        piece + got[:, k * rows : (k + 1) * rows] for k, piece in enumerate((up, own, down))
    )
    from_below = lax.ppermute(up, ROW_COL, partners(-1, False))
    from_above = lax.ppermute(down, ROW_COL, partners(1, False))
    return own + from_below + from_above


def dft_tables(side):
    index = np.arange(side)
    phase = (index[:, None] * index[None, :] % side) * (2.0 * math.pi / side)
    cosine, sine = np.cos(phase) / math.sqrt(side), np.sin(phase) / math.sqrt(side)
    both = np.block([[cosine, sine], [-sine, cosine]])
    out = []
    for table in (both, both.T):
        head = table.astype(jnp.bfloat16)
        out.append((head, (table - head.astype(np.float64)).astype(jnp.bfloat16)))
    return out


def split(x):
    head = x.astype(jnp.bfloat16)
    return head, (x - head.astype(jnp.float32)).astype(jnp.bfloat16)


def right_dot(x, table):
    head, rest = split(x)
    return jnp.dot(
        jnp.concatenate([head, rest, head], axis=1),
        jnp.concatenate([table[0], table[0], table[1]], axis=0),
        preferred_element_type=jnp.float32,
    )


def left_dot(table, x):
    head, rest = split(x)
    return jnp.dot(
        jnp.concatenate([table[0], table[0], table[1]], axis=1),
        jnp.concatenate([head, rest, head], axis=0),
        preferred_element_type=jnp.float32,
    )


def wave_kernel(column, win, probe, amp, forward, inverse, obj, kept, sent, far, factor):
    modes, side = probe.shape[1], probe.shape[2]
    left_col = column[0] == 0
    tiles = side // 8

    def exit_wave(m):
        probe_real = probe[0, m].astype(jnp.float32)
        probe_imag = probe[1, m].astype(jnp.float32)
        exit_real = probe_real * win[0] - probe_imag * win[1]
        exit_imag = probe_real * win[1] + probe_imag * win[0]
        return probe_real, probe_imag, exit_real, exit_imag

    def transform(real, imag, right, left):
        mixed = right_dot(jnp.concatenate([real, imag], axis=1), right)
        return left_dot(left, jnp.concatenate([mixed[:, :side], mixed[:, side:]], axis=0))

    def put(base, first, second):
        where = pl.ds(base, tiles)
        kept[where] = jnp.where(left_col, first, second).reshape((tiles,) + TILE)
        sent[where] = jnp.where(left_col, second, first).reshape((tiles,) + TILE)

    factor[...] = jnp.zeros_like(factor)

    @pl.loop(0, modes)
    def _(m):
        _, _, exit_real, exit_imag = exit_wave(m)
        out = transform(exit_real, exit_imag, inverse, forward)
        far[m] = out
        factor[...] += out[:side] * out[:side] + out[side:] * out[side:]

    factor[...] = amp[...] / (jnp.sqrt(factor[...]) + 0.5)
    obj[...] = jnp.zeros_like(obj)

    @pl.loop(0, modes)
    def _(m):
        scale = factor[...]
        back = transform(far[m, :side] * scale, far[m, side:] * scale, forward, inverse)
        probe_real, probe_imag, exit_real, exit_imag = exit_wave(m)
        diff_real = back[:side] - exit_real
        diff_imag = back[side:] - exit_imag
        obj[0] += probe_real * diff_real + probe_imag * diff_imag
        obj[1] += probe_real * diff_imag - probe_imag * diff_real
        obj[2] += probe_real * probe_real + probe_imag * probe_imag
        grad_real = win[0] * diff_real + win[1] * diff_imag
        grad_imag = win[0] * diff_imag - win[1] * diff_real
        for half in range(side // 128):
            cols = slice(128 * half, 128 * half + 128)
            put((m * (side // 128) + half) * tiles, grad_real[:, cols], grad_imag[:, cols])

    weight = win[0] * win[0] + win[1] * win[1]
    put(modes * (side // 128) * tiles, weight[:, :128], weight[:, 128:])


def waves(column, window, probe, amplitude):
    modes, side = probe.shape[1], probe.shape[2]
    assert side == 256
    forward, inverse = (jnp.asarray(np.stack(table)) for table in dft_tables(side))
    flops = 4 * modes * 2 * side * (6 * side) * (2 * side)
    half = jax.ShapeDtypeStruct(((2 * modes + 1) * (side // 8),) + TILE, jnp.float32)
    vmem = pl.BlockSpec(memory_space=pltpu.VMEM)
    return pl.pallas_call(
        wave_kernel,
        name="waves",
        out_shape=(jax.ShapeDtypeStruct((3, side, side), jnp.float32), half, half),
        in_specs=[pl.BlockSpec(memory_space=pltpu.SMEM)] + [vmem] * 5,
        out_specs=(vmem, vmem, vmem),
        scratch_shapes=[
            pltpu.VMEM((modes, 2 * side, side), jnp.float32),
            pltpu.VMEM((side, side), jnp.float32),
        ],
        compiler_params=pltpu.CompilerParams(vmem_limit_bytes=40 * 1024 * 1024),
        cost_estimate=pl.CostEstimate(
            flops=flops, bytes_accessed=12 * 1024 * 1024, transcendentals=0
        ),
    )(column, window, probe, amplitude, forward, inverse)


def probe_kernel(column, own, other, probe, out):
    modes, side = probe.shape[1], probe.shape[2]
    left_col = column[0] == 0
    chunk = own.shape[1] - 1
    group = math.gcd(chunk, side // 8)

    def halves(tile):
        where = (tile // chunk, slice(tile % chunk, tile % chunk + group))
        mine, theirs = (ref[where].reshape(8 * group, 128) for ref in (own, other))
        return jnp.where(left_col, mine, theirs), jnp.where(left_col, theirs, mine)

    per_half = side // 8
    groups = per_half // group
    base = 2 * modes * per_half
    weight = [halves(base + j * group) for j in range(groups)]
    peak = functools.reduce(jnp.maximum, [jnp.max(w) for pair in weight for w in pair])
    for j in range(groups):
        rows = slice(8 * group * j, 8 * group * (j + 1))
        for half in range(2):
            inverse = 1.0 / (weight[j][half] + 0.1 * peak)
            cols = slice(128 * half, 128 * half + 128)
            for m in range(modes):
                grads = halves((2 * m + half) * per_half + j * group)
                for part in range(2):
                    out[part, m, rows, cols] = (
                        probe[part, m, rows, cols].astype(jnp.float32) + grads[part] * inverse
                    )


def probe_update(column, own, other, probe):
    vmem = pl.BlockSpec(memory_space=pltpu.VMEM)
    return pl.pallas_call(
        probe_kernel,
        name="probe_update",
        out_shape=jax.ShapeDtypeStruct(probe.shape, jnp.float32),
        in_specs=[pl.BlockSpec(memory_space=pltpu.SMEM)] + [vmem] * 3,
        out_specs=vmem,
        compiler_params=pltpu.CompilerParams(vmem_limit_bytes=40 * 1024 * 1024),
        cost_estimate=pl.CostEstimate(
            flops=4 * probe.size, bytes_accessed=9 * probe.size, transcendentals=0
        ),
    )(column, own, other, probe)


def exchange(chunks, axis):
    return lax.all_to_all(chunks, axis, 0, 0, tiled=True)


def sum_and_peak(kept, sent, local_peak):
    far, near = (lax.axis_size(axis) for axis in ROW)
    swap = [(0, 1), (1, 0)]
    tiles = kept + lax.ppermute(sent, "col", swap)
    tiles = tiles.reshape((near, tiles.shape[0] // near) + TILE)
    tiles = jnp.sum(exchange(tiles, "row_1"), axis=0)
    part = tiles.shape[0] * TILE[0] // far
    rows = jnp.sum(exchange(tiles.reshape(far, part, 128), "row_0"), axis=0)
    spare = jnp.full((TILE[0] - part % TILE[0], 128), local_peak)
    rows = jnp.concatenate([rows, spare])
    got = exchange(jnp.broadcast_to(rows, (far,) + rows.shape), "row_0")
    peak = jnp.full((1,) + TILE, jnp.max(got[:, part:]))
    tiles = jnp.concatenate([got[:, :part].reshape(tiles.shape), peak])
    own = exchange(jnp.broadcast_to(tiles, (near,) + tiles.shape), "row_1")
    other = lax.ppermute(own, "col", swap)
    return own, other, jnp.maximum(jnp.max(own[:, -1]), jnp.max(other[:, -1]))


def update(obj_field, probe_modes, centers, amplitudes):
    tile_rows, tile_cols = obj_field.shape[1:]
    side = probe_modes.shape[2]
    margin = side // 2
    start_row = centers[0, 0] - lax.axis_index(ROW) * tile_rows
    start_col = centers[0, 1] - lax.axis_index("col") * tile_cols
    zero = jnp.zeros((), jnp.int32)
    column = lax.axis_index("col").astype(jnp.int32).reshape(1)
    extended = extended_tile(obj_field, margin)
    window = lax.dynamic_slice(extended, (zero, start_row, start_col), (2, side, side))
    stacked, kept, sent = waves(column, window, probe_modes, amplitudes[0])
    start = jnp.stack([start_row, start_col])
    folded = folded_tile(place(start, column, stacked, tile_rows, tile_cols))
    illumination = folded[2]
    own, other, peak = sum_and_peak(kept, sent, jnp.max(illumination))
    new_object = obj_field + folded[:2] / (illumination + 0.1 * peak)
    return new_object, probe_update(column, own, other, probe_modes)


def solution(mesh):
    split_mesh = Mesh(
        mesh.devices.reshape(
            mesh.shape["angle"], mesh.shape["row"] // NEAR, NEAR, mesh.shape["col"]
        ),
        ANGLE_ROW_COL,
    )
    return jax.shard_map(
        update,
        mesh=split_mesh,
        in_specs=(
            P(None, ANGLE_ROW, "col"),
            P(),
            P(ANGLE_ROW_COL, None),
            P(ANGLE_ROW_COL, None, None),
        ),
        out_specs=(P(None, ANGLE_ROW, "col"), P(None, "angle", None, None)),
        check_vma=False,
    )
```

```python
import functools
import math

import jax
import jax.numpy as jnp
import numpy as np
from jax import lax
from jax.experimental import pallas as pl
from jax.experimental.pallas import tpu as pltpu
from jax.sharding import Mesh
from jax.sharding import PartitionSpec as P


ROW = ("row_0", "row_1")
ROW_COL = ROW + ("col",)
ANGLE_ROW = ("angle",) + ROW
ANGLE_ROW_COL = ANGLE_ROW + ("col",)
NEAR = 8
TILE = (8, 128)


def partners(row_step, swap):
    rows = math.prod(lax.axis_size(axis) for axis in ROW)
    cols = lax.axis_size("col")
    assert cols == 2
    return [
        (row * cols + col, (row + row_step) * cols + (1 - col if swap else col))
        for row in range(rows)
        for col in range(cols)
        if 0 <= row + row_step < rows
    ]


def extended_tile(block, margin):
    rows, cols = block.shape[1:]
    assert rows == margin
    left_col = lax.axis_index("col") == 0
    edge = jnp.where(left_col, block[:, :, cols - margin :], block[:, :, :margin])
    above = lax.ppermute(block, ROW_COL, partners(1, False))
    below = lax.ppermute(block, ROW_COL, partners(-1, False))
    edge_above = lax.ppermute(edge, ROW_COL, partners(1, True))
    edge_below = lax.ppermute(edge, ROW_COL, partners(-1, True))
    beside = lax.ppermute(edge, ROW_COL, partners(0, True))
    middle = jnp.concatenate([above, block, below], axis=1)
    side = jnp.concatenate([edge_above, beside, edge_below], axis=1)
    zero = jnp.zeros_like(side)
    return jnp.concatenate(
        [jnp.where(left_col, zero, side), middle, jnp.where(left_col, side, zero)], axis=2
    )


def settle_kernel(starts, column, own, below, above, spot, tile, side, buffer):
    rows, cols = tile.shape[1:]
    width = spot.shape[1]
    left_col = column[0] == 0
    buffer[...] = jnp.zeros_like(buffer)
    for n, (source, band) in enumerate(((own, 1), (below, 0), (above, 2))):
        shift = lax.rem(starts[n, 1], 128)
        where = pl.ds(pl.multiple_of(starts[n, 1] - shift, 128), width + 128)
        tall = jnp.concatenate([spot[...], jnp.zeros((rows, width), jnp.float32)], axis=0)
        weight = pltpu.roll(tall, starts[n, 0], 0)[band * rows : (band + 1) * rows]
        weight = jnp.where(starts[n, 2] == 1, weight, 0.0)
        for k, piece in enumerate((source[:rows], source[rows : 2 * rows], weight)):
            wide = jnp.concatenate([piece, jnp.zeros((rows, 128), jnp.float32)], axis=1)
            buffer[k, :, where] += pltpu.roll(wide, shift, 1)
    tile[...] = buffer[:, :, rows : rows + cols]
    side[...] = jnp.where(left_col, buffer[:, :, rows + cols :], buffer[:, :, :rows])


def settle(starts, column, own, below, above, spot, rows, cols):
    smem = pl.BlockSpec(memory_space=pltpu.SMEM)
    vmem = pl.BlockSpec(memory_space=pltpu.VMEM)
    tile = jax.ShapeDtypeStruct((3, rows, cols), jnp.float32)
    return pl.pallas_call(
        settle_kernel,
        name="settle",
        out_shape=(tile, jax.ShapeDtypeStruct((3, rows, rows), jnp.float32)),
        in_specs=[smem, smem] + [vmem] * 4,
        out_specs=(vmem, vmem),
        scratch_shapes=[pltpu.VMEM((3, rows, cols + 2 * rows), jnp.float32)],
        compiler_params=pltpu.CompilerParams(vmem_limit_bytes=24 * 1024 * 1024),
        cost_estimate=pl.CostEstimate(
            flops=20 * tile.size, bytes_accessed=12 * tile.size, transcendentals=0
        ),
    )(starts, column, own, below, above, spot)


def folded_tile(start, column, own, up, down, spot, rows, cols):
    below = lax.ppermute(up, ROW_COL, partners(-1, False))
    above = lax.ppermute(down, ROW_COL, partners(1, False))
    tags = [got[2 * rows, :3].astype(jnp.int32) for got in (below, above)]
    starts = jnp.stack([jnp.concatenate([start, jnp.ones((1,), jnp.int32)])] + tags)
    tile, side = settle(starts, column, own, below, above, spot, rows, cols)
    got = lax.ppermute(side, ROW_COL, partners(0, True))
    rest = jnp.zeros(got.shape[:2] + (cols - rows,), got.dtype)
    return tile + jnp.where(
        lax.axis_index("col") == 0,
        jnp.concatenate([rest, got], axis=2),
        jnp.concatenate([got, rest], axis=2),
    )


def dft_tables(side):
    index = np.arange(side)
    phase = (index[:, None] * index[None, :] % side) * (2.0 * math.pi / side)
    cosine, sine = np.cos(phase) / math.sqrt(side), np.sin(phase) / math.sqrt(side)
    both = np.block([[cosine, sine], [-sine, cosine]])
    out = []
    for table in (both, both.T):
        head = table.astype(jnp.bfloat16)
        out.append((head, (table - head.astype(np.float64)).astype(jnp.bfloat16)))
    return out


def split(x):
    head = x.astype(jnp.bfloat16)
    return head, (x - head.astype(jnp.float32)).astype(jnp.bfloat16)


def right_dot(x, table):
    head, rest = split(x)
    return jnp.dot(
        jnp.concatenate([head, rest, head], axis=1),
        jnp.concatenate([table[0], table[0], table[1]], axis=0),
        preferred_element_type=jnp.float32,
    )


def left_dot(table, x):
    head, rest = split(x)
    return jnp.dot(
        jnp.concatenate([table[0], table[0], table[1]], axis=1),
        jnp.concatenate([head, rest, head], axis=0),
        preferred_element_type=jnp.float32,
    )


def wave_kernel(
    start, column, win, probe, amp, forward, inverse, own, up, down, spot, kept, sent, far, factor, obj
):
    modes, side = probe.shape[1], probe.shape[2]
    left_col = column[0] == 0
    tiles = side // 8

    def exit_wave(m):
        probe_real = probe[0, m].astype(jnp.float32)
        probe_imag = probe[1, m].astype(jnp.float32)
        exit_real = probe_real * win[0] - probe_imag * win[1]
        exit_imag = probe_real * win[1] + probe_imag * win[0]
        return probe_real, probe_imag, exit_real, exit_imag

    def transform(real, imag, right, left):
        mixed = right_dot(jnp.concatenate([real, imag], axis=1), right)
        return left_dot(left, jnp.concatenate([mixed[:, :side], mixed[:, side:]], axis=0))

    def put(base, first, second):
        where = pl.ds(base, tiles)
        kept[where] = jnp.where(left_col, first, second).reshape((tiles,) + TILE)
        sent[where] = jnp.where(left_col, second, first).reshape((tiles,) + TILE)

    factor[...] = jnp.zeros_like(factor)

    @pl.loop(0, modes)
    def _(m):
        _, _, exit_real, exit_imag = exit_wave(m)
        out = transform(exit_real, exit_imag, inverse, forward)
        far[m] = out
        factor[...] += out[:side] * out[:side] + out[side:] * out[side:]

    factor[...] = amp[...] / (jnp.sqrt(factor[...]) + 0.5)
    obj[...] = jnp.zeros_like(obj)
    spot[...] = jnp.zeros_like(spot)

    @pl.loop(0, modes)
    def _(m):
        scale = factor[...]
        back = transform(far[m, :side] * scale, far[m, side:] * scale, forward, inverse)
        probe_real, probe_imag, exit_real, exit_imag = exit_wave(m)
        diff_real = back[:side] - exit_real
        diff_imag = back[side:] - exit_imag
        obj[0] += probe_real * diff_real + probe_imag * diff_imag
        obj[1] += probe_real * diff_imag - probe_imag * diff_real
        spot[...] += probe_real * probe_real + probe_imag * probe_imag
        grad_real = win[0] * diff_real + win[1] * diff_imag
        grad_imag = win[0] * diff_imag - win[1] * diff_real
        for half in range(side // 128):
            cols = slice(128 * half, 128 * half + 128)
            put((m * (side // 128) + half) * tiles, grad_real[:, cols], grad_imag[:, cols])

    weight = win[0] * win[0] + win[1] * win[1]
    put(modes * (side // 128) * tiles, weight[:, :128], weight[:, 128:])
    rows = side // 2
    for k in range(2):
        tall = jnp.concatenate([obj[k], jnp.zeros((rows, side), jnp.float32)], axis=0)
        tall = pltpu.roll(tall, start[0], 0)
        for band, out in enumerate((up, own, down)):
            out[k * rows : (k + 1) * rows] = tall[band * rows : (band + 1) * rows]
    lane = lax.broadcasted_iota(jnp.int32, (8, side), 1)
    tag = jnp.where(lane == 0, start[0], jnp.where(lane == 1, start[1], 1)).astype(jnp.float32)
    up[2 * rows :] = tag
    down[2 * rows :] = tag


def waves(start, column, window, probe, amplitude):
    modes, side = probe.shape[1], probe.shape[2]
    assert side == 256
    forward, inverse = (jnp.asarray(np.stack(table)) for table in dft_tables(side))
    flops = 4 * modes * 2 * side * (6 * side) * (2 * side)
    half = jax.ShapeDtypeStruct(((2 * modes + 1) * (side // 8),) + TILE, jnp.float32)
    square = jax.ShapeDtypeStruct((side, side), jnp.float32)
    band = jax.ShapeDtypeStruct((side + 8, side), jnp.float32)
    vmem = pl.BlockSpec(memory_space=pltpu.VMEM)
    return pl.pallas_call(
        wave_kernel,
        name="waves",
        out_shape=(square, band, band, square, half, half),
        in_specs=[pl.BlockSpec(memory_space=pltpu.SMEM)] * 2 + [vmem] * 5,
        out_specs=(vmem,) * 6,
        scratch_shapes=[
            pltpu.VMEM((modes, 2 * side, side), jnp.float32),
            pltpu.VMEM((side, side), jnp.float32),
            pltpu.VMEM((2, side, side), jnp.float32),
        ],
        compiler_params=pltpu.CompilerParams(vmem_limit_bytes=40 * 1024 * 1024),
        cost_estimate=pl.CostEstimate(
            flops=flops, bytes_accessed=12 * 1024 * 1024, transcendentals=0
        ),
    )(start, column, window, probe, amplitude, forward, inverse)


def probe_kernel(column, own, other, probe, out):
    modes, side = probe.shape[1], probe.shape[2]
    left_col = column[0] == 0
    chunk = own.shape[1] - 1
    group = math.gcd(chunk, side // 8)

    def halves(tile):
        where = (tile // chunk, slice(tile % chunk, tile % chunk + group))
        mine, theirs = (ref[where].reshape(8 * group, 128) for ref in (own, other))
        return jnp.where(left_col, mine, theirs), jnp.where(left_col, theirs, mine)

    per_half = side // 8
    groups = per_half // group
    base = 2 * modes * per_half
    weight = [halves(base + j * group) for j in range(groups)]
    peak = functools.reduce(jnp.maximum, [jnp.max(w) for pair in weight for w in pair])
    for j in range(groups):
        rows = slice(8 * group * j, 8 * group * (j + 1))
        for half in range(2):
            inverse = 1.0 / (weight[j][half] + 0.1 * peak)
            cols = slice(128 * half, 128 * half + 128)
            for m in range(modes):
                grads = halves((2 * m + half) * per_half + j * group)
                for part in range(2):
                    out[part, m, rows, cols] = (
                        probe[part, m, rows, cols].astype(jnp.float32) + grads[part] * inverse
                    )


def probe_update(column, own, other, probe):
    vmem = pl.BlockSpec(memory_space=pltpu.VMEM)
    return pl.pallas_call(
        probe_kernel,
        name="probe_update",
        out_shape=jax.ShapeDtypeStruct(probe.shape, jnp.float32),
        in_specs=[pl.BlockSpec(memory_space=pltpu.SMEM)] + [vmem] * 3,
        out_specs=vmem,
        compiler_params=pltpu.CompilerParams(vmem_limit_bytes=40 * 1024 * 1024),
        cost_estimate=pl.CostEstimate(
            flops=4 * probe.size, bytes_accessed=9 * probe.size, transcendentals=0
        ),
    )(column, own, other, probe)


def exchange(chunks, axis):
    return lax.all_to_all(chunks, axis, 0, 0, tiled=True)


def sum_and_peak(kept, sent, local_peak):
    far, near = (lax.axis_size(axis) for axis in ROW)
    swap = [(0, 1), (1, 0)]
    tiles = kept + lax.ppermute(sent, "col", swap)
    tiles = tiles.reshape((near, tiles.shape[0] // near) + TILE)
    tiles = jnp.sum(exchange(tiles, "row_1"), axis=0)
    part = tiles.shape[0] * TILE[0] // far
    rows = jnp.sum(exchange(tiles.reshape(far, part, 128), "row_0"), axis=0)
    spare = jnp.full((TILE[0] - part % TILE[0], 128), local_peak)
    rows = jnp.concatenate([rows, spare])
    got = exchange(jnp.broadcast_to(rows, (far,) + rows.shape), "row_0")
    peak = jnp.full((1,) + TILE, jnp.max(got[:, part:]))
    tiles = jnp.concatenate([got[:, :part].reshape(tiles.shape), peak])
    own = exchange(jnp.broadcast_to(tiles, (near,) + tiles.shape), "row_1")
    other = lax.ppermute(own, "col", swap)
    return own, other, jnp.maximum(jnp.max(own[:, -1]), jnp.max(other[:, -1]))


def update(obj_field, probe_modes, centers, amplitudes):
    tile_rows, tile_cols = obj_field.shape[1:]
    side = probe_modes.shape[2]
    margin = side // 2
    start_row = centers[0, 0] - lax.axis_index(ROW) * tile_rows
    start_col = centers[0, 1] - lax.axis_index("col") * tile_cols
    zero = jnp.zeros((), jnp.int32)
    column = lax.axis_index("col").astype(jnp.int32).reshape(1)
    extended = extended_tile(obj_field, margin)
    window = lax.dynamic_slice(extended, (zero, start_row, start_col), (2, side, side))
    start = jnp.stack([start_row, start_col])
    assert side == 2 * tile_rows == 256
    own, up, down, spot, kept, sent = waves(start, column, window, probe_modes, amplitudes[0])
    folded = folded_tile(start, column, own, up, down, spot, tile_rows, tile_cols)
    illumination = folded[2]
    own, other, peak = sum_and_peak(kept, sent, jnp.max(illumination))
    new_object = obj_field + folded[:2] / (illumination + 0.1 * peak)
    return new_object, probe_update(column, own, other, probe_modes)


def solution(mesh):
    split_mesh = Mesh(
        mesh.devices.reshape(
            mesh.shape["angle"], mesh.shape["row"] // NEAR, NEAR, mesh.shape["col"]
        ),
        ANGLE_ROW_COL,
    )
    return jax.shard_map(
        update,
        mesh=split_mesh,
        in_specs=(
            P(None, ANGLE_ROW, "col"),
            P(),
            P(ANGLE_ROW_COL, None),
            P(ANGLE_ROW_COL, None, None),
        ),
        out_specs=(P(None, ANGLE_ROW, "col"), P(None, "angle", None, None)),
        check_vma=False,
    )
```

```python
import functools
import math

import jax
import jax.numpy as jnp
import numpy as np
from jax import lax
from jax.experimental import pallas as pl
from jax.experimental.pallas import tpu as pltpu
from jax.sharding import Mesh
from jax.sharding import PartitionSpec as P


ROW = ("row_0", "row_1", "row_2")
ROW_COL = ROW + ("col",)
ANGLE_ROW = ("angle",) + ROW
ANGLE_ROW_COL = ANGLE_ROW + ("col",)
NEAR, MIDDLE = 4, 4
TILE = (8, 128)


def partners(row_step, swap):
    rows = math.prod(lax.axis_size(axis) for axis in ROW)
    cols = lax.axis_size("col")
    assert cols == 2
    return [
        (row * cols + col, (row + row_step) * cols + (1 - col if swap else col))
        for row in range(rows)
        for col in range(cols)
        if 0 <= row + row_step < rows
    ]


def extended_tile(block, margin):
    rows, cols = block.shape[1:]
    assert rows == margin
    left_col = lax.axis_index("col") == 0
    edge = jnp.where(left_col, block[:, :, cols - margin :], block[:, :, :margin])
    above = lax.ppermute(block, ROW_COL, partners(1, False))
    below = lax.ppermute(block, ROW_COL, partners(-1, False))
    edge_above = lax.ppermute(edge, ROW_COL, partners(1, True))
    edge_below = lax.ppermute(edge, ROW_COL, partners(-1, True))
    beside = lax.ppermute(edge, ROW_COL, partners(0, True))
    middle = jnp.concatenate([above, block, below], axis=1)
    side = jnp.concatenate([edge_above, beside, edge_below], axis=1)
    zero = jnp.zeros_like(side)
    return jnp.concatenate(
        [jnp.where(left_col, zero, side), middle, jnp.where(left_col, side, zero)], axis=2
    )


def settle_kernel(starts, column, own, below, above, spot, tile, side, buffer):
    rows, cols = tile.shape[1:]
    width = spot.shape[1]
    left_col = column[0] == 0
    buffer[...] = jnp.zeros_like(buffer)
    for n, (source, band) in enumerate(((own, 1), (below, 0), (above, 2))):
        shift = lax.rem(starts[n, 1], 128)
        where = pl.ds(pl.multiple_of(starts[n, 1] - shift, 128), width + 128)
        tall = jnp.concatenate([spot[...], jnp.zeros((rows, width), jnp.float32)], axis=0)
        weight = pltpu.roll(tall, starts[n, 0], 0)[band * rows : (band + 1) * rows]
        weight = jnp.where(starts[n, 2] == 1, weight, 0.0)
        for k, piece in enumerate((source[:rows], source[rows : 2 * rows], weight)):
            wide = jnp.concatenate([piece, jnp.zeros((rows, 128), jnp.float32)], axis=1)
            buffer[k, :, where] += pltpu.roll(wide, shift, 1)
    tile[...] = buffer[:, :, rows : rows + cols]
    side[...] = jnp.where(left_col, buffer[:, :, rows + cols :], buffer[:, :, :rows])


def settle(starts, column, own, below, above, spot, rows, cols):
    smem = pl.BlockSpec(memory_space=pltpu.SMEM)
    vmem = pl.BlockSpec(memory_space=pltpu.VMEM)
    tile = jax.ShapeDtypeStruct((3, rows, cols), jnp.float32)
    return pl.pallas_call(
        settle_kernel,
        name="settle",
        out_shape=(tile, jax.ShapeDtypeStruct((3, rows, rows), jnp.float32)),
        in_specs=[smem, smem] + [vmem] * 4,
        out_specs=(vmem, vmem),
        scratch_shapes=[pltpu.VMEM((3, rows, cols + 2 * rows), jnp.float32)],
        compiler_params=pltpu.CompilerParams(vmem_limit_bytes=24 * 1024 * 1024),
        cost_estimate=pl.CostEstimate(
            flops=20 * tile.size, bytes_accessed=12 * tile.size, transcendentals=0
        ),
    )(starts, column, own, below, above, spot)


def folded_tile(start, column, own, up, down, spot, rows, cols):
    below = lax.ppermute(up, ROW_COL, partners(-1, False))
    above = lax.ppermute(down, ROW_COL, partners(1, False))
    tags = [got[2 * rows, :3].astype(jnp.int32) for got in (below, above)]
    starts = jnp.stack([jnp.concatenate([start, jnp.ones((1,), jnp.int32)])] + tags)
    tile, side = settle(starts, column, own, below, above, spot, rows, cols)
    got = lax.ppermute(side, ROW_COL, partners(0, True))
    rest = jnp.zeros(got.shape[:2] + (cols - rows,), got.dtype)
    return tile + jnp.where(
        lax.axis_index("col") == 0,
        jnp.concatenate([rest, got], axis=2),
        jnp.concatenate([got, rest], axis=2),
    )


def dft_tables(side):
    index = np.arange(side)
    phase = (index[:, None] * index[None, :] % side) * (2.0 * math.pi / side)
    cosine, sine = np.cos(phase) / math.sqrt(side), np.sin(phase) / math.sqrt(side)
    both = np.block([[cosine, sine], [-sine, cosine]])
    out = []
    for table in (both, both.T):
        head = table.astype(jnp.bfloat16)
        out.append((head, (table - head.astype(np.float64)).astype(jnp.bfloat16)))
    return out


def split(x):
    head = x.astype(jnp.bfloat16)
    return head, (x - head.astype(jnp.float32)).astype(jnp.bfloat16)


def right_dot(x, table):
    head, rest = split(x)
    return jnp.dot(
        jnp.concatenate([head, rest, head], axis=1),
        jnp.concatenate([table[0], table[0], table[1]], axis=0),
        preferred_element_type=jnp.float32,
    )


def left_dot(table, x):
    head, rest = split(x)
    return jnp.dot(
        jnp.concatenate([table[0], table[0], table[1]], axis=1),
        jnp.concatenate([head, rest, head], axis=0),
        preferred_element_type=jnp.float32,
    )


def wave_kernel(
    start, column, win, probe, amp, forward, inverse, own, up, down, spot, kept, sent, far, factor, obj
):
    modes, side = probe.shape[1], probe.shape[2]
    left_col = column[0] == 0
    tiles = side // 8

    def exit_wave(m):
        probe_real = probe[0, m].astype(jnp.float32)
        probe_imag = probe[1, m].astype(jnp.float32)
        exit_real = probe_real * win[0] - probe_imag * win[1]
        exit_imag = probe_real * win[1] + probe_imag * win[0]
        return probe_real, probe_imag, exit_real, exit_imag

    def transform(real, imag, right, left):
        mixed = right_dot(jnp.concatenate([real, imag], axis=1), right)
        return left_dot(left, jnp.concatenate([mixed[:, :side], mixed[:, side:]], axis=0))

    def put(base, first, second):
        where = pl.ds(base, tiles)
        kept[where] = jnp.where(left_col, first, second).reshape((tiles,) + TILE)
        sent[where] = jnp.where(left_col, second, first).reshape((tiles,) + TILE)

    factor[...] = jnp.zeros_like(factor)

    @pl.loop(0, modes)
    def _(m):
        _, _, exit_real, exit_imag = exit_wave(m)
        out = transform(exit_real, exit_imag, inverse, forward)
        far[m] = out
        factor[...] += out[:side] * out[:side] + out[side:] * out[side:]

    factor[...] = amp[...] / (jnp.sqrt(factor[...]) + 0.5)
    obj[...] = jnp.zeros_like(obj)
    spot[...] = jnp.zeros_like(spot)

    @pl.loop(0, modes)
    def _(m):
        scale = factor[...]
        back = transform(far[m, :side] * scale, far[m, side:] * scale, forward, inverse)
        probe_real, probe_imag, exit_real, exit_imag = exit_wave(m)
        diff_real = back[:side] - exit_real
        diff_imag = back[side:] - exit_imag
        obj[0] += probe_real * diff_real + probe_imag * diff_imag
        obj[1] += probe_real * diff_imag - probe_imag * diff_real
        spot[...] += probe_real * probe_real + probe_imag * probe_imag
        grad_real = win[0] * diff_real + win[1] * diff_imag
        grad_imag = win[0] * diff_imag - win[1] * diff_real
        for half in range(side // 128):
            cols = slice(128 * half, 128 * half + 128)
            put((m * (side // 128) + half) * tiles, grad_real[:, cols], grad_imag[:, cols])

    weight = win[0] * win[0] + win[1] * win[1]
    put(modes * (side // 128) * tiles, weight[:, :128], weight[:, 128:])
    rows = side // 2
    for k in range(2):
        tall = jnp.concatenate([obj[k], jnp.zeros((rows, side), jnp.float32)], axis=0)
        tall = pltpu.roll(tall, start[0], 0)
        for band, out in enumerate((up, own, down)):
            out[k * rows : (k + 1) * rows] = tall[band * rows : (band + 1) * rows]
    lane = lax.broadcasted_iota(jnp.int32, (8, side), 1)
    tag = jnp.where(lane == 0, start[0], jnp.where(lane == 1, start[1], 1)).astype(jnp.float32)
    up[2 * rows :] = tag
    down[2 * rows :] = tag


def waves(start, column, window, probe, amplitude):
    modes, side = probe.shape[1], probe.shape[2]
    assert side == 256
    forward, inverse = (jnp.asarray(np.stack(table)) for table in dft_tables(side))
    flops = 4 * modes * 2 * side * (6 * side) * (2 * side)
    half = jax.ShapeDtypeStruct(((2 * modes + 1) * (side // 8),) + TILE, jnp.float32)
    square = jax.ShapeDtypeStruct((side, side), jnp.float32)
    band = jax.ShapeDtypeStruct((side + 8, side), jnp.float32)
    vmem = pl.BlockSpec(memory_space=pltpu.VMEM)
    return pl.pallas_call(
        wave_kernel,
        name="waves",
        out_shape=(square, band, band, square, half, half),
        in_specs=[pl.BlockSpec(memory_space=pltpu.SMEM)] * 2 + [vmem] * 5,
        out_specs=(vmem,) * 6,
        scratch_shapes=[
            pltpu.VMEM((modes, 2 * side, side), jnp.float32),
            pltpu.VMEM((side, side), jnp.float32),
            pltpu.VMEM((2, side, side), jnp.float32),
        ],
        compiler_params=pltpu.CompilerParams(vmem_limit_bytes=40 * 1024 * 1024),
        cost_estimate=pl.CostEstimate(
            flops=flops, bytes_accessed=12 * 1024 * 1024, transcendentals=0
        ),
    )(start, column, window, probe, amplitude, forward, inverse)


def probe_kernel(column, own, other, probe, out):
    modes, side = probe.shape[1], probe.shape[2]
    left_col = column[0] == 0
    chunk = own.shape[1] - 1
    group = math.gcd(chunk, side // 8)

    def halves(tile):
        where = (tile // chunk, slice(tile % chunk, tile % chunk + group))
        mine, theirs = (ref[where].reshape(8 * group, 128) for ref in (own, other))
        return jnp.where(left_col, mine, theirs), jnp.where(left_col, theirs, mine)

    per_half = side // 8
    groups = per_half // group
    base = 2 * modes * per_half
    weight = [halves(base + j * group) for j in range(groups)]
    peak = functools.reduce(jnp.maximum, [jnp.max(w) for pair in weight for w in pair])
    for j in range(groups):
        rows = slice(8 * group * j, 8 * group * (j + 1))
        for half in range(2):
            inverse = 1.0 / (weight[j][half] + 0.1 * peak)
            cols = slice(128 * half, 128 * half + 128)
            for m in range(modes):
                grads = halves((2 * m + half) * per_half + j * group)
                for part in range(2):
                    out[part, m, rows, cols] = (
                        probe[part, m, rows, cols].astype(jnp.float32) + grads[part] * inverse
                    )


def probe_update(column, own, other, probe):
    vmem = pl.BlockSpec(memory_space=pltpu.VMEM)
    return pl.pallas_call(
        probe_kernel,
        name="probe_update",
        out_shape=jax.ShapeDtypeStruct(probe.shape, jnp.float32),
        in_specs=[pl.BlockSpec(memory_space=pltpu.SMEM)] + [vmem] * 3,
        out_specs=vmem,
        compiler_params=pltpu.CompilerParams(vmem_limit_bytes=40 * 1024 * 1024),
        cost_estimate=pl.CostEstimate(
            flops=4 * probe.size, bytes_accessed=9 * probe.size, transcendentals=0
        ),
    )(column, own, other, probe)


def exchange(chunks, axis):
    return lax.all_to_all(chunks, axis, 0, 0, tiled=True)


def sum_and_peak(kept, sent, local_peak):
    swap = [(0, 1), (1, 0)]
    tiles = kept + lax.ppermute(sent, "col", swap)
    for axis in ROW[:0:-1]:
        count = lax.axis_size(axis)
        tiles = tiles.reshape((count, tiles.shape[0] // count) + TILE)
        tiles = jnp.sum(exchange(tiles, axis), axis=0)
    far = lax.axis_size(ROW[0])
    part = tiles.shape[0] * TILE[0] // far
    rows = jnp.sum(exchange(tiles.reshape(far, part, 128), ROW[0]), axis=0)
    seen = lax.ppermute(jnp.full(TILE, local_peak), "col", swap)
    local_peak = jnp.maximum(local_peak, jnp.max(seen))
    spare = jnp.full((TILE[0] - part % TILE[0], 128), local_peak)
    rows = jnp.concatenate([rows, spare])
    got = exchange(jnp.broadcast_to(rows, (far,) + rows.shape), ROW[0])
    peak = jnp.max(got[:, part:])
    tiles = got[:, :part].reshape(tiles.shape)
    for axis in ROW[1:]:
        tiles = jnp.concatenate([tiles, jnp.full((1,) + TILE, peak)])
        tiles = jnp.broadcast_to(tiles, (lax.axis_size(axis),) + tiles.shape)
        own = exchange(tiles, axis)
        peak = jnp.max(own[:, -1])
        tiles = own[:, :-1].reshape((-1,) + TILE)
    other = lax.ppermute(own, "col", swap)
    return own, other, peak


def update(obj_field, probe_modes, centers, amplitudes):
    tile_rows, tile_cols = obj_field.shape[1:]
    side = probe_modes.shape[2]
    margin = side // 2
    start_row = centers[0, 0] - lax.axis_index(ROW) * tile_rows
    start_col = centers[0, 1] - lax.axis_index("col") * tile_cols
    zero = jnp.zeros((), jnp.int32)
    column = lax.axis_index("col").astype(jnp.int32).reshape(1)
    extended = extended_tile(obj_field, margin)
    window = lax.dynamic_slice(extended, (zero, start_row, start_col), (2, side, side))
    start = jnp.stack([start_row, start_col])
    assert side == 2 * tile_rows == 256
    own, up, down, spot, kept, sent = waves(start, column, window, probe_modes, amplitudes[0])
    folded = folded_tile(start, column, own, up, down, spot, tile_rows, tile_cols)
    illumination = folded[2]
    own, other, peak = sum_and_peak(kept, sent, jnp.max(illumination))
    new_object = obj_field + folded[:2] / (illumination + 0.1 * peak)
    return new_object, probe_update(column, own, other, probe_modes)


def solution(mesh):
    split_mesh = Mesh(
        mesh.devices.reshape(
            mesh.shape["angle"],
            mesh.shape["row"] // (NEAR * MIDDLE),
            MIDDLE,
            NEAR,
            mesh.shape["col"],
        ),
        ANGLE_ROW_COL,
    )
    return jax.shard_map(
        update,
        mesh=split_mesh,
        in_specs=(
            P(None, ANGLE_ROW, "col"),
            P(),
            P(ANGLE_ROW_COL, None),
            P(ANGLE_ROW_COL, None, None),
        ),
        out_specs=(P(None, ANGLE_ROW, "col"), P(None, "angle", None, None)),
        check_vma=False,
    )
```
